8 devices in a mesh: dp: 1 (over z), fsdp: 8 (over y, x, core).
Axes of the slice: x: 2, y: 2, z: 1, core: 2. Of those that a mesh axis runs over, the one named last changes fastest.
Arguments:
- hidden: bfloat16 [2, 8192, 1024], P(None, ('dp', 'fsdp'))
- targets: int32 [2, 8192], P(None, ('dp', 'fsdp'))
- w_out: bfloat16 [50304, 1024], P('fsdp')
Outputs:
- output 1: float32 [2], P('dp')
- output 2: float32 [2, 8192, 1024], P(None, ('dp', 'fsdp'))
- output 3: float32 [50304, 1024], P(('dp', 'fsdp'))
All inputs are finite; a program needn't handle non-finite values.
Results may differ from the reference program's by a relative error of at most 0.001.
Values are sent between devices in bfloat16 or wider.
A program may use at most 1 GiB of HBM per device.

```python
import jax
import jax.numpy as jnp
from jax import lax

TOK_DEV = 1024
GROUP_SIZE = 8
VOCAB_SIZE = 50304
MODEL_DIM = 1024

TOKENS_PART = TOK_DEV * GROUP_SIZE
VOCAB_BLK = VOCAB_SIZE // GROUP_SIZE


def setup_inputs(seed: int = 0, part: int = 0) -> dict:
    base_key = jax.random.key(seed)
    shared_key, parts_key = jax.random.split(base_key)
    part_key = jax.random.fold_in(parts_key, part)
    key_hid, key_tgt = jax.random.split(part_key)
    hidden = jax.random.normal(key_hid, (2, TOKENS_PART, MODEL_DIM), jnp.float32).astype(jnp.bfloat16)
    targets = jax.random.randint(key_tgt, (2, TOKENS_PART), 0, VOCAB_SIZE, jnp.int32)
    targets = targets.at[0, 0].set(0).at[1, TOKENS_PART - 1].set(VOCAB_SIZE - 1)
    w_scaled = jax.random.normal(shared_key, (VOCAB_SIZE, MODEL_DIM), jnp.float32) * MODEL_DIM ** -0.5
    return {'hidden': hidden, 'targets': targets, 'w_out': w_scaled.astype(jnp.bfloat16)}


def reference(hidden, targets, w_out):
    tok_blocks = hidden.reshape(2 * GROUP_SIZE, TOK_DEV, MODEL_DIM)
    tgt_blocks = targets.reshape(2 * GROUP_SIZE, TOK_DEV)
    w_blocks = w_out.reshape(GROUP_SIZE, VOCAB_BLK, MODEL_DIM)
    blk_ids = jnp.arange(GROUP_SIZE, dtype=jnp.int32)
    col_ids = jnp.arange(VOCAB_BLK, dtype=jnp.int32)[None, :]

    def block_logits(tok_rows, row_tgt, w_blk, blk_idx):
        logits = jnp.dot(tok_rows, w_blk.T, preferred_element_type=jnp.float32)
        tgt_hit = (row_tgt - blk_idx * VOCAB_BLK)[:, None] == col_ids
        return logits, tgt_hit

    def token_stats(blk_in):
        tok_rows, row_tgt = blk_in

        def vocab_step(run_stats, w_in):
            run_max, run_sum, tgt_logit = run_stats
            logits, tgt_hit = block_logits(tok_rows, row_tgt, w_in[0], w_in[1])
            tgt_logit = tgt_logit + jnp.sum(jnp.where(tgt_hit, logits, 0.0), axis=1)
            new_max = jnp.maximum(run_max, jnp.max(logits, axis=1))
            run_sum = run_sum * jnp.exp(run_max - new_max) + jnp.sum(jnp.exp(logits - new_max[:, None]), axis=1)
            return (new_max, run_sum, tgt_logit), None

        init_stats = (jnp.full((TOK_DEV,), -jnp.inf, jnp.float32), jnp.zeros((TOK_DEV,), jnp.float32), jnp.zeros((TOK_DEV,), jnp.float32))
        (run_max, run_sum, tgt_logit), _ = lax.scan(vocab_step, init_stats, (w_blocks, blk_ids))
        return run_max + jnp.log(run_sum), tgt_logit

    log_norm, tgt_logit = lax.map(token_stats, (tok_blocks, tgt_blocks))
    loss_vals = jnp.sum((log_norm - tgt_logit).reshape(2, TOKENS_PART), axis=1) / TOKENS_PART

    def token_grads(d_w, blk_in):
        tok_rows, row_tgt, row_norm = blk_in

        def vocab_step(d_rows, w_in):
            logits, tgt_hit = block_logits(tok_rows, row_tgt, w_in[0], w_in[1])
            soft_probs = jnp.exp(logits - row_norm[:, None])
            d_logits = ((soft_probs - tgt_hit.astype(jnp.float32)) / TOKENS_PART).astype(jnp.bfloat16)
            d_rows = d_rows + jnp.dot(d_logits, w_in[0], preferred_element_type=jnp.float32)
            d_w_blk = jnp.dot(d_logits.T, tok_rows, preferred_element_type=jnp.float32)
            return d_rows, d_w_blk

        d_rows, d_w_blocks = lax.scan(vocab_step, jnp.zeros((TOK_DEV, MODEL_DIM), jnp.float32), (w_blocks, blk_ids))
        return d_w + d_w_blocks.reshape(VOCAB_SIZE, MODEL_DIM), d_rows

    d_w, d_rows = lax.scan(token_grads, jnp.zeros((VOCAB_SIZE, MODEL_DIM), jnp.float32), (tok_blocks, tgt_blocks, log_norm))
    return loss_vals, d_rows.reshape(2, TOKENS_PART, MODEL_DIM), d_w
```

```python
import functools

import jax
import jax.numpy as jnp
from jax import lax
from jax.experimental import pallas as pl
from jax.experimental.pallas import tpu as pltpu
from jax.sharding import PartitionSpec as P


VMEM_LIMIT = 63 * 1024 * 1024
NT = (((1,), (1,)), ((), ()))
TN = (((0,), (0,)), ((), ()))
CORE, X, Y = 1, 2, 4

GROUPS = (((0, 0), (0, 1)), ((1, 0), (1, 1)), ((2, 1), (4, 0), (3, 1), (5, 0)),
          ((2, 0), (4, 1), (3, 0), (5, 1)), ((6, 0), (6, 1), (7, 0), (7, 1)))
BLOCKS = tuple(blk for group in GROUPS for blk in group)
SLOT = {blk: i for i, blk in enumerate(BLOCKS)}


def spans(size, step):
    n = max(1, (size + step // 2) // step)
    edges = [i * step for i in range(n)] + [size]
    return [slice(a, b) for a, b in zip(edges, edges[1:])]


def params(n_axes):
    return pltpu.CompilerParams(dimension_semantics=("arbitrary",) * n_axes, vmem_limit_bytes=VMEM_LIMIT)


def logits_kernel(v_tile, n_blk, tgt_ref, w_ref, *rest):
    z_ref, h_ref, st_ref = rest[-3:]
    v, m = pl.program_id(0), pl.program_id(1)
    tok = h_ref.shape[1]

    @pl.when(jnp.logical_and(v == 0, m == 0))
    def _():
        for i in range(n_blk):
            h_ref[i] = rest[i][...]

    @pl.when(v == 0)
    def _():
        st_ref[m, 0] = jnp.full((8, tok), -jnp.inf, jnp.float32)
        st_ref[m, 1] = jnp.zeros((8, tok), jnp.float32)
        st_ref[m, 2] = jnp.zeros((8, tok), jnp.float32)

    for rows in spans(v_tile, 512):
        n = (rows.stop - rows.start) // 8
        for cols in spans(tok, 512):
            width = cols.stop - cols.start
            z = lax.dot_general(w_ref[rows], h_ref[m, cols], NT, preferred_element_type=jnp.float32)
            z_ref[0, rows, cols] = z
            z = z.reshape(n, 8, width)
            old_max = st_ref[m, 0, :, cols]
            new_max = jnp.maximum(old_max, jnp.max(z, axis=0))
            st_ref[m, 0, :, cols] = new_max
            st_ref[m, 1, :, cols] = (st_ref[m, 1, :, cols] * jnp.exp(old_max - new_max)
                                     + jnp.sum(jnp.exp(z - new_max[None]), axis=0))
            hit = st_ref[m, 2, :, cols]
            want = tgt_ref[m, :, cols] - (v * v_tile + rows.start) - lax.broadcasted_iota(jnp.int32, (8, width), 0)
            for i in range(n):
                hit = jnp.where(want == 8 * i, z[i], hit)
            st_ref[m, 2, :, cols] = hit


def logits_call(group, tgt, w, h, filled, v_tile):
    tok, d = h[0].shape
    vocab = w.shape[0]
    n, total = len(h), len(BLOCKS)
    at = SLOT[group[0]] // n
    ins = ([pl.BlockSpec((n, 1, tok), lambda v, m: (0, 0, 0)), pl.BlockSpec((v_tile, d), lambda v, m: (v, 0))]
           + [pl.BlockSpec((tok, d), lambda v, m: (0, 0), pipeline_mode=pl.Buffered(1))] * n
           + [pl.BlockSpec(memory_space=pl.ANY)] * len(filled))
    return pl.pallas_call(
        functools.partial(logits_kernel, v_tile, n),
        grid=(vocab // v_tile, n),
        in_specs=ins,
        out_specs=[pl.BlockSpec((1, v_tile, tok), lambda v, m: (n * at + m, v, 0)),
                   pl.BlockSpec((n, tok, d), lambda v, m: (at, 0, 0), pipeline_mode=pl.Buffered(1)),
                   pl.BlockSpec((n, 3, 8, tok), lambda v, m: (at, 0, 0, 0))],
        out_shape=(jax.ShapeDtypeStruct((total, vocab, tok), jnp.float32),
                   jax.ShapeDtypeStruct((total, tok, d), jnp.bfloat16),
                   jax.ShapeDtypeStruct((total, 3, 8, tok), jnp.float32)),
        input_output_aliases={2 + n + i: i for i in range(len(filled))},
        compiler_params=params(2),
        cost_estimate=pl.CostEstimate(flops=2 * n * tok * d * vocab, bytes_accessed=4 * n * tok * vocab, transcendentals=0),
        name="logits",
    )(tgt, w, *h, *filled)


def d_logits(z, norm, at_tgt, tgt, base):
    rows, tok = z.shape
    prob = jnp.exp(z - norm).astype(jnp.bfloat16)
    want = jnp.clip(tgt - base, -1, rows).astype(jnp.int16)
    ids = lax.broadcasted_iota(jnp.int16, (rows, tok), 0)
    return jnp.where(ids == jnp.broadcast_to(want, (rows, tok)),
                     jnp.broadcast_to(at_tgt.astype(jnp.bfloat16), (rows, tok)), prob)


def dh_kernel(v_tile, n_v, vocab, n_init, scale, norm_ref, at_ref, tgt_ref, z_ref, w_ref, *rest):
    inits, outs, (acc_ref, dz_ref) = rest[:2 * n_init], rest[2 * n_init:-2], rest[-2:]
    u = pl.program_id(0)
    step, blk = lax.div(u - 1, 2), lax.rem(u - 1, 2)
    cur, prev = lax.rem(u, 2), lax.rem(u + 1, 2)
    base = jnp.minimum(lax.div(u, 2) * v_tile, vocab - v_tile)
    again = n_v * v_tile - vocab
    _, d, tok = acc_ref.shape

    def make(rows):
        dz_ref[cur, rows] = d_logits(z_ref[0, rows], norm_ref[0], at_ref[0], tgt_ref[0], base + rows.start)

    pieces = spans(v_tile, 320)

    @pl.when(u == 0)
    def _():
        for rows in pieces:
            make(rows)

    @pl.when(jnp.logical_and(u > 0, step == n_v - 1))
    def _():
        dz_ref[prev, :again] = jnp.zeros((again, tok), dz_ref.dtype)

    @pl.when(jnp.logical_and(u > 0, step == 0))
    def _():
        acc_ref[blk] = jnp.zeros((d, tok), jnp.float32)

    @pl.when(u > 0)
    def _():
        todo = list(pieces)
        for rows in spans(d, 512):
            for cols in spans(tok, 512):
                acc_ref[blk, rows, cols] += lax.dot_general(w_ref[:, rows], dz_ref[prev, :, cols], TN,
                                                            preferred_element_type=jnp.float32)
                if todo:
                    make(todo.pop(0))

    for b in range(2):
        if n_init:
            part = inits[0].shape[0]

            @pl.when(jnp.logical_and(jnp.logical_and(u > 0, blk == b), step * part < d))
            def _():
                rows = pl.ds(pl.multiple_of(step * part, part), part)
                total = acc_ref[b, rows, :]
                for ref in inits[b * n_init:(b + 1) * n_init]:
                    total = total + ref[...]
                acc_ref[b, rows, :] = total

        @pl.when(jnp.logical_and(jnp.logical_and(u > 0, blk == b), step == n_v - 1))
        def _():
            if scale is None:
                outs[b][...] = acc_ref[b]
            else:
                outs[0][b] = acc_ref[b].T * scale


def dh_call(pair, norm, at_tgt, tgt, z_all, w, inits0, inits1, v_tile, scale=None):
    _, vocab, tok = z_all.shape
    d = w.shape[1]
    n_v = pl.cdiv(vocab, v_tile)
    s0, s1 = SLOT[pair[0]], SLOT[pair[1]]
    n_init = len(inits0)
    part = d // 4
    nxt = lambda u: jnp.minimum(u, 2 * n_v - 1)
    prv = lambda u: jnp.maximum(u - 1, 0)
    slot = lambda u: jnp.where(lax.rem(nxt(u), 2) == 0, s0, s1)
    tile = lambda u: pl.multiple_of(jnp.minimum(lax.div(u, 2) * v_tile, vocab - v_tile), 16)
    row = pl.BlockSpec((1, 1, tok), lambda u: (slot(u), 0, 0))
    init = pl.BlockSpec((part, tok), lambda u: (jnp.minimum(lax.div(prv(u), 2), 3), 0))
    if scale is None:
        out_specs = [pl.BlockSpec((d, tok), lambda u: (0, 0))] * 2
        out_shape = [jax.ShapeDtypeStruct((d, tok), jnp.float32)] * 2
    else:
        out_specs = [pl.BlockSpec((2, tok, d), lambda u: (0, 0, 0))]
        out_shape = [jax.ShapeDtypeStruct((2, tok, d), jnp.float32)]
    return pl.pallas_call(
        functools.partial(dh_kernel, v_tile, n_v, vocab, n_init, scale),
        grid=(2 * n_v + 1,),
        in_specs=[row, row, row,
                  pl.BlockSpec((pl.Element(1), pl.Element(v_tile), pl.Element(tok)), lambda u: (slot(u), tile(nxt(u)), 0)),
                  pl.BlockSpec((pl.Element(v_tile), pl.Element(d)), lambda u: (tile(prv(u)), 0))] + [init] * (2 * n_init),
        out_specs=out_specs,
        out_shape=out_shape,
        scratch_shapes=[pltpu.VMEM((2, d, tok), jnp.float32), pltpu.VMEM((2, v_tile, tok), jnp.bfloat16)],
        compiler_params=params(1),
        cost_estimate=pl.CostEstimate(flops=4 * tok * d * vocab, bytes_accessed=8 * tok * vocab, transcendentals=0),
        name="d_hidden",
    )(norm, at_tgt, tgt, z_all, w, *inits0, *inits1)


def dw_kernel(v_tile, n_t, scale, norm_ref, at_ref, tgt_ref, z_ref, h_ref, out_ref, dz_ref):
    u = pl.program_id(0)
    cur, prev = lax.rem(u, 2), lax.rem(u + 1, 2)
    base = lax.div(u, n_t) * v_tile

    def make(rows, cols):
        dz_ref[cur, rows, cols] = d_logits(z_ref[0, rows, cols], norm_ref[0, :, cols], at_ref[0, :, cols],
                                           tgt_ref[0, :, cols], base + rows.start)

    pieces = [(rows, cols) for rows in spans(v_tile, 512) for cols in spans(z_ref.shape[2], 512)]

    @pl.when(u == 0)
    def _():
        for rows, cols in pieces:
            make(rows, cols)

    @pl.when(lax.rem(u, n_t) == 1)
    def _():
        out_ref[...] = jnp.zeros_like(out_ref)

    @pl.when(u > 0)
    def _():
        for rows, cols in pieces:
            out_ref[rows, cols] += jnp.dot(dz_ref[prev, rows], h_ref[0, :, cols], preferred_element_type=jnp.float32)
            make(rows, cols)

    @pl.when(jnp.logical_and(u > 0, lax.rem(u, n_t) == 0))
    def _():
        out_ref[...] = out_ref[...] * scale


def dw_call(norm, at_tgt, tgt, z_all, h_all, scale, v_tile):
    n_t, vocab, tok = z_all.shape
    d = h_all.shape[2]
    assert tok == d
    units = vocab // v_tile * n_t
    nxt = lambda u: jnp.minimum(u, units - 1)
    prv = lambda u: jnp.maximum(u - 1, 0)
    row = pl.BlockSpec((1, 1, tok), lambda u: (lax.rem(nxt(u), n_t), 0, 0))
    return pl.pallas_call(
        functools.partial(dw_kernel, v_tile, n_t, scale),
        grid=(units + 1,),
        in_specs=[row, row, row,
                  pl.BlockSpec((1, v_tile, tok), lambda u: (lax.rem(nxt(u), n_t), lax.div(nxt(u), n_t), 0)),
                  pl.BlockSpec((1, tok, d), lambda u: (lax.rem(prv(u), n_t), 0, 0))],
        out_specs=pl.BlockSpec((v_tile, d), lambda u: (lax.div(prv(u), n_t), 0)),
        out_shape=jax.ShapeDtypeStruct((vocab, d), jnp.float32),
        scratch_shapes=[pltpu.VMEM((2, v_tile, tok), jnp.bfloat16)],
        compiler_params=params(1),
        cost_estimate=pl.CostEstimate(flops=2 * n_t * tok * d * vocab, bytes_accessed=4 * n_t * tok * vocab, transcendentals=0),
        name="d_w",
    )(norm, at_tgt, tgt, z_all, h_all)


def solution(mesh):
    group_size = mesh.shape['fsdp']
    assert group_size == 8

    def swap(x, mask):
        return lax.ppermute(x, 'fsdp', [(i, i ^ mask) for i in range(group_size)])

    def after(x, *deps):
        return lax.optimization_barrier((x, *deps))[0]

    def local_head(hidden, targets, w_loc):
        n_micro, tok, d = hidden.shape
        vocab = w_loc.shape[0]
        tokens = tok * group_size
        me = lax.axis_index('fsdp')

        t = {0: targets}
        for mask in (CORE, X, Y, X ^ Y):
            t[mask] = swap(targets, mask)
        h = {(0, 0): hidden[0], (0, 1): hidden[1]}
        over_x, over_y, _ = lax.optimization_barrier((hidden, hidden, (t[X], t[Y], t[X ^ Y])))
        h[2, 1], h[4, 0] = swap(over_x[1], X), swap(over_y[0], Y)
        h[2, 0], h[4, 1] = swap(after(over_x[0], h[2, 1]), X), swap(after(over_y[1], h[4, 0]), Y)
        h[1, 0], h[1, 1] = swap(h[0, 0], CORE), swap(h[0, 1], CORE)
        h[6, 0], h[6, 1] = swap(after(h[4, 0], h[2, 0]), X), swap(after(h[2, 1], h[4, 1]), Y)
        for mask in (3, 5, 7):
            for m in range(2):
                h[mask, m] = swap(h[mask - 1, m], CORE)
        t[3], t[5], t[7] = swap(jnp.stack([t[2], t[4], t[6]]), CORE)

        filled, tgt = (), []
        for group in GROUPS:
            tgt.append((jnp.stack([t[mask][m] for mask, m in group]) - me * vocab)[:, None])
            filled = logits_call(group, tgt[-1], w_loc, [h[blk] for blk in group], filled, vocab // 3)
        z_all, h_all, stats = filled
        tgt = jnp.concatenate(tgt)

        run_max = jnp.max(stats[:, 0], axis=1)
        run_sum = jnp.sum(stats[:, 1] * jnp.exp(stats[:, 0] - run_max[:, None]), axis=1)
        tgt_logit = jnp.sum(stats[:, 2], axis=1)
        hits = jnp.stack([sum(jnp.sum(tgt_logit[SLOT[mask, m]]) for mask in range(8)) for m in range(2)])
        for mask in (CORE, X, Y):
            mine = jnp.concatenate([jnp.stack([run_max, run_sum]), jnp.broadcast_to(hits[:, None, None], (2, 1, tok))], axis=1)
            other = swap(mine, mask)
            hits = hits + other[:, -1, 0]
            other = jnp.stack([other[:, SLOT[blk[0] ^ mask, blk[1]]] for blk in BLOCKS], axis=1)
            new_max = jnp.maximum(run_max, other[0])
            run_sum = run_sum * jnp.exp(run_max - new_max) + other[1] * jnp.exp(other[0] - new_max)
            run_max = new_max
        norm = run_max + jnp.log(run_sum)
        at_tgt = (jnp.exp(tgt_logit - norm) - 1.0)[:, None]
        norm_sum = jnp.sum(norm, axis=1)
        norm_sum = jnp.stack([jnp.stack([norm_sum[SLOT[mask, m]] for m in range(2)]) for mask in range(8)])
        for _ in range(3):
            norm_sum = norm_sum[0::2] + norm_sum[1::2]
        loss_vals = (norm_sum[0] - hits) / tokens

        norm = norm[:, None]
        v_tile = 1280

        came = {blk: [] for blk in BLOCKS}
        last = None

        def partial(a, b, scale=None):
            nonlocal norm, last
            if last is not None:
                norm = after(norm, last)
            out = dh_call((a, b), norm, at_tgt, tgt, z_all, w_loc, came[a], came[b], v_tile, scale)
            last = out[0]
            return out

        def send(blk, value, mask):
            came[blk[0] ^ mask, blk[1]].append(swap(value, mask))

        def to_core(a, b):
            for blk, value in zip((a, b), partial(a, b)):
                send(blk, value, CORE)

        def to_links(a, b):
            for blk, value, mask in zip((a, b), partial(a, b), (X, Y)):
                send(blk, value, mask)

        to_core((7, 0), (7, 1))
        to_core((3, 0), (5, 1))
        to_links((6, 0), (6, 1))
        to_core((3, 1), (5, 0))
        to_links((2, 0), (4, 1))
        to_core((1, 0), (1, 1))
        to_links((2, 1), (4, 0))
        norm = after(norm, last)
        d_w = dw_call(norm, at_tgt, tgt, z_all, h_all, 1.0 / tokens, vocab // 3)
        last = d_w
        d_rows, = partial((0, 0), (0, 1), 1.0 / tokens)
        return loss_vals, d_rows, d_w

    return jax.shard_map(local_head, mesh=mesh,
                         in_specs=(P(None, ('dp', 'fsdp'), None), P(None, ('dp', 'fsdp')), P('fsdp', None)),
                         out_specs=(P('dp'), P(None, ('dp', 'fsdp'), None), P(('dp', 'fsdp'), None)),
                         check_vma=False)
```

```python
import functools

import jax
import jax.numpy as jnp
from jax import lax
from jax.experimental import pallas as pl
from jax.experimental.pallas import tpu as pltpu
from jax.sharding import PartitionSpec as P


HOIST_LOGITS, HOIST_DH, HOIST_DW = 512, 64, 8
VMEM_LIMIT = 63 * 1024 * 1024
NT = (((1,), (1,)), ((), ()))
TN = (((0,), (0,)), ((), ()))
CORE, X, Y = 1, 2, 4

GROUPS = (((0, 0), (0, 1)), ((1, 0), (1, 1)), ((2, 1), (4, 0), (3, 1), (5, 0)),
          ((2, 0), (4, 1), (3, 0), (5, 1)), ((6, 0), (6, 1), (7, 0), (7, 1)))
BLOCKS = tuple(blk for group in GROUPS for blk in group)
SLOT = {blk: i for i, blk in enumerate(BLOCKS)}


def spans(size, step):
    n = max(1, (size + step // 2) // step)
    edges = [i * step for i in range(n)] + [size]
    return [slice(a, b) for a, b in zip(edges, edges[1:])]


def params(n_axes, hoist):
    return pltpu.CompilerParams(dimension_semantics=("arbitrary",) * n_axes, vmem_limit_bytes=VMEM_LIMIT)


def logits_kernel(v_tile, n_blk, tgt_ref, w_ref, *rest):
    z_ref, h_ref, st_ref = rest[-3:]
    v, m = pl.program_id(0), pl.program_id(1)
    tok = h_ref.shape[1]

    @pl.when(jnp.logical_and(v == 0, m == 0))
    def _():
        for i in range(n_blk):
            h_ref[i] = rest[i][...]

    @pl.when(v == 0)
    def _():
        st_ref[m, 0] = jnp.full((8, tok), -jnp.inf, jnp.float32)
        st_ref[m, 1] = jnp.zeros((8, tok), jnp.float32)
        st_ref[m, 2] = jnp.zeros((8, tok), jnp.float32)

    for rows in spans(v_tile, 512):
        n = (rows.stop - rows.start) // 8
        for cols in spans(tok, 512):
            width = cols.stop - cols.start
            z = lax.dot_general(w_ref[rows], h_ref[m, cols], NT, preferred_element_type=jnp.float32)
            z_ref[0, rows, cols] = z
            z = z.reshape(n, 8, width)
            old_max = st_ref[m, 0, :, cols]
            new_max = jnp.maximum(old_max, jnp.max(z, axis=0))
            st_ref[m, 0, :, cols] = new_max
            st_ref[m, 1, :, cols] = (st_ref[m, 1, :, cols] * jnp.exp(old_max - new_max)
                                     + jnp.sum(jnp.exp(z - new_max[None]), axis=0))
            hit = st_ref[m, 2, :, cols]
            want = tgt_ref[m, :, cols] - (v * v_tile + rows.start) - lax.broadcasted_iota(jnp.int32, (8, width), 0)
            for i in range(n):
                hit = jnp.where(want == 8 * i, z[i], hit)
            st_ref[m, 2, :, cols] = hit


def logits_call(group, tgt, w, h, filled, v_tile):
    tok, d = h[0].shape
    vocab = w.shape[0]
    n, total = len(h), len(BLOCKS)
    at = SLOT[group[0]] // n
    ins = ([pl.BlockSpec((n, 1, tok), lambda v, m: (0, 0, 0)), pl.BlockSpec((v_tile, d), lambda v, m: (v, 0))]
           + [pl.BlockSpec((tok, d), lambda v, m: (0, 0), pipeline_mode=pl.Buffered(1))] * n
           + [pl.BlockSpec(memory_space=pl.ANY)] * len(filled))
    return pl.pallas_call(
        functools.partial(logits_kernel, v_tile, n),
        grid=(vocab // v_tile, n),
        in_specs=ins,
        out_specs=[pl.BlockSpec((1, v_tile, tok), lambda v, m: (n * at + m, v, 0)),
                   pl.BlockSpec((n, tok, d), lambda v, m: (at, 0, 0), pipeline_mode=pl.Buffered(1)),
                   pl.BlockSpec((n, 3, 8, tok), lambda v, m: (at, 0, 0, 0))],
        out_shape=(jax.ShapeDtypeStruct((total, vocab, tok), jnp.float32),
                   jax.ShapeDtypeStruct((total, tok, d), jnp.bfloat16),
                   jax.ShapeDtypeStruct((total, 3, 8, tok), jnp.float32)),
        input_output_aliases={2 + n + i: i for i in range(len(filled))},
        compiler_params=params(2, HOIST_LOGITS),
        cost_estimate=pl.CostEstimate(flops=2 * n * tok * d * vocab, bytes_accessed=4 * n * tok * vocab, transcendentals=0),
        name="logits",
    )(tgt, w, *h, *filled)


def d_logits(z, norm, at_tgt, tgt, base):
    rows, tok = z.shape
    prob = jnp.exp(z - norm).astype(jnp.bfloat16)
    want = jnp.clip(tgt - base, -1, rows).astype(jnp.int16)
    ids = lax.broadcasted_iota(jnp.int16, (rows, tok), 0)
    return jnp.where(ids == jnp.broadcast_to(want, (rows, tok)),
                     jnp.broadcast_to(at_tgt.astype(jnp.bfloat16), (rows, tok)), prob)


def dh_kernel(v_tile, n_v, vocab, n_init, scale, norm_ref, at_ref, tgt_ref, z_ref, w_ref, *rest):
    inits, outs, (acc_ref, dz_ref) = rest[:2 * n_init], rest[2 * n_init:-2], rest[-2:]
    u = pl.program_id(0)
    step, blk = lax.div(u - 1, 2), lax.rem(u - 1, 2)
    cur, prev = lax.rem(u, 2), lax.rem(u + 1, 2)
    base = jnp.minimum(lax.div(u, 2) * v_tile, vocab - v_tile)
    again = n_v * v_tile - vocab
    _, d, tok = acc_ref.shape

    def make(rows):
        dz_ref[cur, rows] = d_logits(z_ref[0, rows], norm_ref[0], at_ref[0], tgt_ref[0], base + rows.start)

    pieces = spans(v_tile, 320)

    @pl.when(u == 0)
    def _():
        for rows in pieces:
            make(rows)

    @pl.when(jnp.logical_and(u > 0, step == n_v - 1))
    def _():
        dz_ref[prev, :again] = jnp.zeros((again, tok), dz_ref.dtype)

    @pl.when(jnp.logical_and(u > 0, step == 0))
    def _():
        acc_ref[blk] = jnp.zeros((d, tok), jnp.float32)

    @pl.when(u > 0)
    def _():
        todo = list(pieces)
        for rows in spans(d, 512):
            for cols in spans(tok, 512):
                acc_ref[blk, rows, cols] += lax.dot_general(w_ref[:, rows], dz_ref[prev, :, cols], TN,
                                                            preferred_element_type=jnp.float32)
                if todo:
                    make(todo.pop(0))

    for b in range(2):
        if n_init:
            part = inits[0].shape[0]

            @pl.when(jnp.logical_and(jnp.logical_and(u > 0, blk == b), step * part < d))
            def _():
                rows = pl.ds(pl.multiple_of(step * part, part), part)
                total = acc_ref[b, rows, :]
                for ref in inits[b * n_init:(b + 1) * n_init]:
                    total = total + ref[...]
                acc_ref[b, rows, :] = total

        @pl.when(jnp.logical_and(jnp.logical_and(u > 0, blk == b), step == n_v - 1))
        def _():
            if scale is None:
                outs[b][...] = acc_ref[b]
            else:
                outs[0][b] = acc_ref[b].T * scale


def dh_call(pair, norm, at_tgt, tgt, z_all, w, inits0, inits1, v_tile, scale=None):
    _, vocab, tok = z_all.shape
    d = w.shape[1]
    n_v = pl.cdiv(vocab, v_tile)
    s0, s1 = SLOT[pair[0]], SLOT[pair[1]]
    n_init = len(inits0)
    part = d // 4
    nxt = lambda u: jnp.minimum(u, 2 * n_v - 1)
    prv = lambda u: jnp.maximum(u - 1, 0)
    slot = lambda u: jnp.where(lax.rem(nxt(u), 2) == 0, s0, s1)
    tile = lambda u: pl.multiple_of(jnp.minimum(lax.div(u, 2) * v_tile, vocab - v_tile), 16)
    row = pl.BlockSpec((1, 1, tok), lambda u: (slot(u), 0, 0))
    init = pl.BlockSpec((part, tok), lambda u: (jnp.minimum(lax.div(prv(u), 2), 3), 0))
    if scale is None:
        out_specs = [pl.BlockSpec((d, tok), lambda u: (0, 0))] * 2
        out_shape = [jax.ShapeDtypeStruct((d, tok), jnp.float32)] * 2
    else:
        out_specs = [pl.BlockSpec((2, tok, d), lambda u: (0, 0, 0))]
        out_shape = [jax.ShapeDtypeStruct((2, tok, d), jnp.float32)]
    return pl.pallas_call(
        functools.partial(dh_kernel, v_tile, n_v, vocab, n_init, scale),
        grid=(2 * n_v + 1,),
        in_specs=[row, row, row,
                  pl.BlockSpec((pl.Element(1), pl.Element(v_tile), pl.Element(tok)), lambda u: (slot(u), tile(nxt(u)), 0)),
                  pl.BlockSpec((pl.Element(v_tile), pl.Element(d)), lambda u: (tile(prv(u)), 0))] + [init] * (2 * n_init),
        out_specs=out_specs,
        out_shape=out_shape,
        scratch_shapes=[pltpu.VMEM((2, d, tok), jnp.float32), pltpu.VMEM((2, v_tile, tok), jnp.bfloat16)],
        compiler_params=params(1, HOIST_DH),
        cost_estimate=pl.CostEstimate(flops=4 * tok * d * vocab, bytes_accessed=8 * tok * vocab, transcendentals=0),
        name="d_hidden",
    )(norm, at_tgt, tgt, z_all, w, *inits0, *inits1)


def dw_kernel(v_tile, n_t, scale, norm_ref, at_ref, tgt_ref, z_ref, h_ref, out_ref, dz_ref):
    u = pl.program_id(0)
    cur, prev = lax.rem(u, 2), lax.rem(u + 1, 2)
    base = lax.div(u, n_t) * v_tile

    def make(rows, cols):
        dz_ref[cur, rows, cols] = d_logits(z_ref[0, rows, cols], norm_ref[0, :, cols], at_ref[0, :, cols],
                                           tgt_ref[0, :, cols], base + rows.start)

    pieces = [(rows, cols) for rows in spans(v_tile, 512) for cols in spans(z_ref.shape[2], 512)]

    @pl.when(u == 0)
    def _():
        for rows, cols in pieces:
            make(rows, cols)

    @pl.when(lax.rem(u, n_t) == 1)
    def _():
        out_ref[...] = jnp.zeros_like(out_ref)

    @pl.when(u > 0)
    def _():
        for rows, cols in pieces:
            out_ref[rows, cols] += jnp.dot(dz_ref[prev, rows], h_ref[0, :, cols], preferred_element_type=jnp.float32)
            make(rows, cols)

    @pl.when(jnp.logical_and(u > 0, lax.rem(u, n_t) == 0))
    def _():
        out_ref[...] = out_ref[...] * scale


def dw_call(norm, at_tgt, tgt, z_all, h_all, scale, v_tile):
    n_t, vocab, tok = z_all.shape
    d = h_all.shape[2]
    assert tok == d
    units = vocab // v_tile * n_t
    nxt = lambda u: jnp.minimum(u, units - 1)
    prv = lambda u: jnp.maximum(u - 1, 0)
    row = pl.BlockSpec((1, 1, tok), lambda u: (lax.rem(nxt(u), n_t), 0, 0))
    return pl.pallas_call(
        functools.partial(dw_kernel, v_tile, n_t, scale),
        grid=(units + 1,),
        in_specs=[row, row, row,
                  pl.BlockSpec((1, v_tile, tok), lambda u: (lax.rem(nxt(u), n_t), lax.div(nxt(u), n_t), 0)),
                  pl.BlockSpec((1, tok, d), lambda u: (lax.rem(prv(u), n_t), 0, 0))],
        out_specs=pl.BlockSpec((v_tile, d), lambda u: (lax.div(prv(u), n_t), 0)),
        out_shape=jax.ShapeDtypeStruct((vocab, d), jnp.float32),
        scratch_shapes=[pltpu.VMEM((2, v_tile, tok), jnp.bfloat16)],
        compiler_params=params(1, HOIST_DW),
        cost_estimate=pl.CostEstimate(flops=2 * n_t * tok * d * vocab, bytes_accessed=4 * n_t * tok * vocab, transcendentals=0),
        name="d_w",
    )(norm, at_tgt, tgt, z_all, h_all)


def solution(mesh):
    group_size = mesh.shape['fsdp']
    assert group_size == 8

    def swap(x, mask):
        return lax.ppermute(x, 'fsdp', [(i, i ^ mask) for i in range(group_size)])

    def after(x, *deps):
        return lax.optimization_barrier((x, *deps))[0]

    def local_head(hidden, targets, w_loc):
        n_micro, tok, d = hidden.shape
        vocab = w_loc.shape[0]
        tokens = tok * group_size
        me = lax.axis_index('fsdp')

        t = {0: targets}
        for mask in (CORE, X, Y, X ^ Y):
            t[mask] = swap(targets, mask)
        h = {(0, 0): hidden[0], (0, 1): hidden[1]}
        sent = lax.optimization_barrier((h[0, 0], h[0, 1], t[X], t[Y], t[X ^ Y]))[:2]
        h[2, 1], h[4, 0] = swap(sent[1], X), swap(sent[0], Y)
        h[2, 0], h[4, 1] = swap(after(sent[0], h[2, 1]), X), swap(after(sent[1], h[4, 0]), Y)
        h[1, 0], h[1, 1] = swap(h[0, 0], CORE), swap(h[0, 1], CORE)
        h[6, 0], h[6, 1] = swap(after(h[4, 0], h[2, 0]), X), swap(after(h[2, 1], h[4, 1]), Y)
        for mask in (3, 5, 7):
            for m in range(2):
                h[mask, m] = swap(h[mask - 1, m], CORE)
        t[3], t[5], t[7] = swap(jnp.stack([t[2], t[4], t[6]]), CORE)

        filled, tgt = (), []
        for group in GROUPS:
            tgt.append((jnp.stack([t[mask][m] for mask, m in group]) - me * vocab)[:, None])
            filled = logits_call(group, tgt[-1], w_loc, [h[blk] for blk in group], filled, vocab // 3)
        z_all, h_all, stats = filled
        tgt = jnp.concatenate(tgt)

        run_max = jnp.max(stats[:, 0], axis=1)
        run_sum = jnp.sum(stats[:, 1] * jnp.exp(stats[:, 0] - run_max[:, None]), axis=1)
        tgt_logit = jnp.sum(stats[:, 2], axis=1)
        hits = jnp.stack([sum(jnp.sum(tgt_logit[SLOT[mask, m]]) for mask in range(8)) for m in range(2)])
        for mask in (CORE, X, Y):
            mine = jnp.concatenate([jnp.stack([run_max, run_sum]), jnp.broadcast_to(hits[:, None, None], (2, 1, tok))], axis=1)
            other = swap(mine, mask)
            hits = hits + other[:, -1, 0]
            other = jnp.stack([other[:, SLOT[blk[0] ^ mask, blk[1]]] for blk in BLOCKS], axis=1)
            new_max = jnp.maximum(run_max, other[0])
            run_sum = run_sum * jnp.exp(run_max - new_max) + other[1] * jnp.exp(other[0] - new_max)
            run_max = new_max
        norm = run_max + jnp.log(run_sum)
        at_tgt = (jnp.exp(tgt_logit - norm) - 1.0)[:, None]
        norm_sum = jnp.sum(norm, axis=1)
        norm_sum = jnp.stack([jnp.stack([norm_sum[SLOT[mask, m]] for m in range(2)]) for mask in range(8)])
        for _ in range(3):
            norm_sum = norm_sum[0::2] + norm_sum[1::2]
        loss_vals = (norm_sum[0] - hits) / tokens

        norm = norm[:, None]
        v_tile = 1280

        came = {blk: [] for blk in BLOCKS}
        last = None

        def partial(a, b, scale=None):
            nonlocal norm, last
            if last is not None:
                norm = after(norm, last)
            out = dh_call((a, b), norm, at_tgt, tgt, z_all, w_loc, came[a], came[b], v_tile, scale)
            last = out[0]
            return out

        def send(blk, value, mask):
            came[blk[0] ^ mask, blk[1]].append(swap(value, mask))

        def to_core(a, b):
            for blk, value in zip((a, b), partial(a, b)):
                send(blk, value, CORE)

        def to_links(a, b):
            for blk, value, mask in zip((a, b), partial(a, b), (X, Y)):
                send(blk, value, mask)

        to_core((7, 0), (7, 1))
        to_core((3, 0), (5, 1))
        to_links((6, 0), (6, 1))
        to_core((3, 1), (5, 0))
        to_links((2, 0), (4, 1))
        to_core((1, 0), (1, 1))
        to_links((2, 1), (4, 0))
        norm = after(norm, last)
        d_w = dw_call(norm, at_tgt, tgt, z_all, h_all, 1.0 / tokens, vocab // 3)
        last = d_w
        d_rows, = partial((0, 0), (0, 1), 1.0 / tokens)
        return loss_vals, d_rows, d_w

    return jax.shard_map(local_head, mesh=mesh,
                         in_specs=(P(None, ('dp', 'fsdp'), None), P(None, ('dp', 'fsdp')), P('fsdp', None)),
                         out_specs=(P('dp'), P(None, ('dp', 'fsdp'), None), P(('dp', 'fsdp'), None)),
                         check_vma=False)
```
